32 devices in a mesh: dom: 32 (over z, y, x, core).
Axes of the slice: x: 2, y: 2, z: 4, core: 2. Of those that a mesh axis runs over, the one named last changes fastest.
Arguments:
- forcing: float32 [1024, 128], P('dom'), may hold values from -6 to 6
- first_guess: float32 [1024, 128], P('dom'), may hold values from -4 to 4
- corners: int32 [3, 262144], P(None, 'dom'), may hold values from 0 to 8191, as said below
- gradients: float32 [4, 262144], P(None, 'dom'), may hold values from -5 to 5
- element_area: float32 [262144], P('dom'), may hold values from 0.5 to 2
- element_depth: float32 [262144], P('dom'), may hold values from 0.2 to 4
- send_blocks: int32 [32, 4, 8], P('dom'), may hold values from 0 to 32, as said below
- recv_blocks: int32 [32, 4, 8], P('dom'), may hold values from 0 to 32, as said below
Outputs:
- elevation: float32 [1024, 128], P('dom')
- residual_left: float32 [1024, 128], P('dom')
The draws below stay inside these ranges and needn't reach their ends.
Inputs may be any that keep to these rules, and one draw needn't show every extreme that they name: `corners`: column e of device d's elements names three different local nodes of device d, numbered below (64) * 128: numbers below 4096 are its owned nodes in block order, the rest its halo blocks. The first corner is an owned node, and every owned node is the first corner of some element of its device. `send_blocks`: entry [d, o, s] is the owned block of device d sent in slot s of offset o to the reader d - k_o, or 32 for an empty slot; it is live exactly when recv_blocks[d - k_o, o, s] is, and readers outside the mesh get nothing. Live blocks of one device and offset differ. For k_o = 1 every slot toward an existing reader is live. `recv_blocks`: entry [q, o, s] is the halo block of device q filled by slot s of offset o from device q + k_o, or 32 for an empty slot. The live entries of one device differ.
All inputs are finite; a program needn't handle non-finite values.
Results may differ from the reference program's by a relative error of at most 0.00022.
Values sent between devices are 32-bit elements; how exact they have to be, the bound alone decides.
No kernel may reach another device: no remote copies, remote signals or barrier semaphores. Data moves between devices by JAX's collectives and lax.ppermute only.
A program may use at most 64 MiB of HBM per device.

```python
import math
import jax
import jax.numpy as jnp

BLOCK = 128
OWN_BLOCKS = 32
SLOTS = 8
REACH = 2
ITERS = 2
OFFSETS = 4
HALO_BLOCKS = 32
ELEM_DEV = 8192
NODES = 131072
ELEMS = 262144
N_DOM = 32


def shift_values():
    return jnp.array([shift_at - REACH if shift_at < REACH else shift_at - REACH + 1 for shift_at in range(OFFSETS)], dtype=jnp.int32)


def link_tables(key):
    base = jax.random.fold_in(key, 4242)
    key_live, key_start, key_place = jax.random.split(base, 3)
    shift_table = shift_values()
    readers = jnp.arange(N_DOM, dtype=jnp.int32)[:, None, None]
    sources = readers + shift_table[None, :, None]
    inside = (sources >= 0) & (sources < N_DOM)
    coin = jax.random.randint(key_live, (N_DOM, OFFSETS, SLOTS), 0, 4, dtype=jnp.int32)
    forced = jnp.broadcast_to(shift_table[None, :, None] == 1, (N_DOM, OFFSETS, SLOTS))
    live = inside & ((coin != 0) | forced)
    start = jax.random.randint(key_start, (N_DOM, OFFSETS, 1), 0, OWN_BLOCKS, dtype=jnp.int32)
    slot_ids = jnp.arange(SLOTS, dtype=jnp.int32)[None, None, :]
    read_blocks = jnp.where(live, (start + slot_ids) % OWN_BLOCKS, OWN_BLOCKS).astype(jnp.int32)

    def placing(one_key):
        return jax.random.permutation(one_key, HALO_BLOCKS)
    places = jax.vmap(placing)(jax.random.split(key_place, N_DOM)).astype(jnp.int32)
    places = places.reshape(N_DOM, OFFSETS, SLOTS)
    recv_table = jnp.where(live, places, HALO_BLOCKS).astype(jnp.int32)
    owners = jnp.arange(N_DOM, dtype=jnp.int32)[:, None, None]
    targets = owners - shift_table[None, :, None]
    target_in = (targets >= 0) & (targets < N_DOM)
    clipped = jnp.clip(targets, 0, N_DOM - 1).astype(jnp.int32)
    offset_ids = jnp.arange(OFFSETS, dtype=jnp.int32)[None, :, None]
    picked = read_blocks[clipped, offset_ids, slot_ids]
    send_table = jnp.where(target_in, picked, OWN_BLOCKS).astype(jnp.int32)
    return (send_table, recv_table)


def draw_send_blocks(key, part):
    return link_tables(key)[0]


def draw_recv_blocks(key, part):
    return link_tables(key)[1]


def draw_corners(key, part):
    base = jax.random.fold_in(key, 31)
    key_perm, key_first, key_second = jax.random.split(base, 3)
    owned_nodes = OWN_BLOCKS * BLOCK
    local_nodes = (OWN_BLOCKS + HALO_BLOCKS) * BLOCK

    def shuffled(one_key):
        return jax.random.permutation(one_key, ELEM_DEV)
    leading = jax.vmap(shuffled)(jax.random.split(key_perm, N_DOM)).astype(jnp.int32) % owned_nodes
    step_one = jax.random.randint(key_first, (N_DOM, ELEM_DEV), 1, local_nodes, dtype=jnp.int32)
    extra = jax.random.randint(key_second, (N_DOM, ELEM_DEV), 0, local_nodes - 2, dtype=jnp.int32)
    step_two = 1 + (step_one + extra) % (local_nodes - 1)
    stacked = jnp.stack([leading, (leading + step_one) % local_nodes, (leading + step_two) % local_nodes])
    return stacked.reshape(3, N_DOM * ELEM_DEV).astype(jnp.int32)


def block_scale(stream_key, shape, shards, least, top_value):
    factor_of = 1.0
    for axis_at, parts in shards:
        steps = jax.random.uniform(jax.random.fold_in(jax.random.fold_in(stream_key, 6), axis_at), (parts,), jnp.float32, least / len(shards), top_value / len(shards))
        factor_of = factor_of * jnp.repeat(jnp.exp(steps), shape[axis_at] // parts).reshape((-1,) + (1,) * (len(shape) - 1 - axis_at))
    return factor_of


def noise(own_key, dims, spread, reach, shards=(), kind=jnp.bfloat16):
    values = jax.random.normal(own_key, dims, jnp.float32) * spread
    if len(shards) > 0:
        values = block_scale(own_key, dims, shards, -0.22, 0.18) * values
    return jnp.clip(values, min=-reach, max=reach).astype(kind)


def setup_inputs(seed: int = 0) -> dict:
    arg_keys = jax.random.split(jax.random.key(seed), 9)
    return {
        "forcing": noise(arg_keys[0], (N_DOM * OWN_BLOCKS, BLOCK), 1.0, 6.0, ((0, 32),), jnp.float32),
        "first_guess": noise(arg_keys[1], (N_DOM * OWN_BLOCKS, BLOCK), 0.5, 4.0, ((0, 32),), jnp.float32),
        "corners": draw_corners(jax.random.fold_in(arg_keys[8], 71), 0),
        "gradients": noise(arg_keys[3], (4, ELEMS), 1.0, 5.0, ((1, 32),), jnp.float32),
        "element_area": jnp.clip(jnp.exp(math.log(2.0) - 1.3862944 * jax.random.uniform(arg_keys[4], (ELEMS,), jnp.float32) ** block_scale(arg_keys[4], (ELEMS,), ((0, 32),), -0.2, 0.2)), 0.5, 2.0),
        "element_depth": jnp.clip(jnp.exp(math.log(4.0) - 2.9957323 * jax.random.uniform(arg_keys[5], (ELEMS,), jnp.float32) ** block_scale(arg_keys[5], (ELEMS,), ((0, 32),), -0.2, 0.2)), 0.2, 4.0),
        "send_blocks": draw_send_blocks(jax.random.fold_in(arg_keys[8], 71), 0),
        "recv_blocks": draw_recv_blocks(jax.random.fold_in(arg_keys[8], 71), 0),
    }


def shift_list():
    return [shift_at - REACH if shift_at < REACH else shift_at - REACH + 1 for shift_at in range(OFFSETS)]


def node_numbers(corners, send_blocks, recv_blocks):
    shift_table = jnp.array(shift_list(), dtype=jnp.int32)
    readers = jnp.arange(N_DOM, dtype=jnp.int32)[:, None, None]
    sources = readers + shift_table[None, :, None]
    inside = (sources >= 0) & (sources < N_DOM)
    clipped = jnp.clip(sources, 0, N_DOM - 1).astype(jnp.int32)
    offset_ids = jnp.arange(OFFSETS, dtype=jnp.int32)[None, :, None]
    slot_ids = jnp.arange(SLOTS, dtype=jnp.int32)[None, None, :]
    source_block = send_blocks[clipped, offset_ids, slot_ids]
    live = inside & (source_block < OWN_BLOCKS) & (recv_blocks < HALO_BLOCKS)
    nowhere = N_DOM * OWN_BLOCKS
    global_block = jnp.where(live, clipped * OWN_BLOCKS + source_block, nowhere).astype(jnp.int32)
    target = jnp.where(live, recv_blocks, HALO_BLOCKS).astype(jnp.int32)
    readers_full = jnp.broadcast_to(readers, target.shape).astype(jnp.int32)
    halo_table = jnp.full((N_DOM, HALO_BLOCKS + 1), nowhere, dtype=jnp.int32)
    halo_table = halo_table.at[readers_full, target].set(global_block)
    owned_table = (jnp.arange(N_DOM, dtype=jnp.int32)[:, None] * OWN_BLOCKS
                   + jnp.arange(OWN_BLOCKS, dtype=jnp.int32)[None, :])
    block_table = jnp.concatenate([owned_table, halo_table[:, :HALO_BLOCKS]], axis=1)
    owners = (jnp.arange(N_DOM * ELEM_DEV, dtype=jnp.int32) // ELEM_DEV)[None, :]
    mapped = block_table[owners, corners // BLOCK]
    return (mapped * BLOCK + corners % BLOCK).astype(jnp.int32)


def reference(forcing, first_guess, corners, gradients, element_area, element_depth, send_blocks, recv_blocks):
    nodes = node_numbers(corners, send_blocks, recv_blocks)
    grad_x = [gradients[0], gradients[2], -(gradients[0] + gradients[2])]
    grad_y = [gradients[1], gradients[3], -(gradients[1] + gradients[3])]
    scaled = element_depth * element_area
    stiffness = [[scaled * (grad_x[row_at] * grad_x[col_at] + grad_y[row_at] * grad_y[col_at])
                  for col_at in range(3)] for row_at in range(3)]
    flat_nodes = nodes.reshape(-1)
    extent = NODES + BLOCK
    third = element_area / 3.0
    mass = jax.ops.segment_sum(jnp.concatenate([third, third, third]), flat_nodes,
                               num_segments=extent)[:NODES].reshape(forcing.shape)

    def operate(field):
        padded = jnp.concatenate([field.reshape(-1), jnp.zeros((BLOCK,), dtype=jnp.float32)])
        values = [padded[nodes[corner_at]] for corner_at in range(3)]
        contrib = jnp.concatenate([stiffness[row_at][0] * values[0] + stiffness[row_at][1] * values[1]
                                   + stiffness[row_at][2] * values[2] for row_at in range(3)])
        summed = jax.ops.segment_sum(contrib, flat_nodes, num_segments=extent)[:NODES].reshape(field.shape)
        return mass * field + summed

    elevation = first_guess
    residual = forcing - operate(first_guess)
    direction = residual
    norm_now = jnp.sum(residual * residual)
    for step_at in range(ITERS):
        applied = operate(direction)
        step_size = norm_now / jnp.sum(direction * applied)
        elevation = elevation + step_size * direction
        residual = residual - step_size * applied
        norm_next = jnp.sum(residual * residual)
        direction = residual + (norm_next / norm_now) * direction
        norm_now = norm_next
    return elevation, residual
```

```python
import functools

import jax
import jax.numpy as jnp
from jax import lax
from jax.experimental import pallas as pl
from jax.experimental.pallas import tpu as pltpu
from jax.sharding import PartitionSpec as P

ITERS = 2
PIECES = 2
CHUNK = 2048


def paired_swap(block, axis, reach, odd):
    count = lax.axis_size(axis)
    route = []
    for low in range(count - reach):
        if (low // reach) % 2 == odd:
            route += [(low, low + reach), (low + reach, low)]
    return lax.ppermute(block, axis, route)


def shift_list(offsets):
    half_count = offsets // 2
    return [
        shift_at - half_count if shift_at < half_count else shift_at - half_count + 1
        for shift_at in range(offsets)
    ]


def exact_dot(left, right):
    return jnp.dot(left, right, precision=lax.Precision.HIGHEST, preferred_element_type=jnp.float32)


def split(values):
    pieces = []
    for _ in range(PIECES):
        piece = values.astype(jnp.bfloat16)
        pieces.append(piece)
        values = values - piece.astype(jnp.float32)
    return pieces


def rows_hot(table, count):
    return (
        lax.broadcasted_iota(jnp.int32, (count, table.shape[1]), 0) == table
    ).astype(jnp.float32)


def chosen(flag, yes, no):
    return jnp.where(jnp.full(yes.shape, flag, jnp.int32) == 1, yes, no)


def write_messages(flags_ref, packed, toward, refs):
    slots = packed.shape[0] // len(toward)
    to = {t: packed[at * slots : (at + 1) * slots] for at, t in enumerate(toward)}
    up = jnp.concatenate([to[2], to[1]], axis=0)
    down = jnp.concatenate([to[-2], to[-1]], axis=0)
    even_core, even_chip = flags_ref[0], flags_ref[1]
    refs[0][...] = chosen(even_chip, up, down)
    refs[1][...] = chosen(even_chip, down, up)
    refs[2][...] = chosen(even_core, to[1], to[-1])


def read_messages(flags_ref, toward, refs):
    first, second, partner = (ref[...] for ref in refs)
    slots = first.shape[0] // 2
    even_core, even_chip = flags_ref[0], flags_ref[1]
    near, far = partner[:slots], partner[slots:]
    got = {
        2: chosen(even_chip, second[:slots], first[:slots]),
        -2: chosen(even_chip, first[:slots], second[:slots]),
        1: chosen(even_core, far, near),
        -1: chosen(even_core, near, far),
    }
    return jnp.concatenate([got[t] for t in toward], axis=0)


def pack_kernel(shifts, flags_ref, x_ref, send_ref, *out_refs):
    hot = rows_hot(send_ref[...], x_ref.shape[0])
    packed = exact_dot(hot.T, x_ref[...])
    write_messages(flags_ref, packed, [-k for k in shifts], out_refs)


def apply_kernel(
    chunk, shifts, flags_ref, x_ref, recv_ref, corners_ref, grad_ref, area_ref, depth_ref, *rest
):
    in_refs, own_ref, out_refs = rest[:3], rest[3], rest[4:]
    own, columns = x_ref.shape
    halo = recv_ref.shape[1]
    blocks = own + halo
    shift = columns.bit_length() - 1
    recv_hot = rows_hot(recv_ref[...], halo)
    incoming = read_messages(flags_ref, [-k for k in shifts], in_refs)
    field = jnp.concatenate([x_ref[...], exact_dot(recv_hot, incoming)], axis=0)
    field_pieces = split(field.T)
    tables = [
        jnp.concatenate([piece[:, :height] for piece in field_pieces], axis=1)
        for height in (own, blocks)
    ]
    block_ids = lax.broadcasted_iota(jnp.int32, (blocks, chunk), 0)
    lane_ids = lax.broadcasted_iota(jnp.int32, (columns, chunk), 0)

    def step(at, accs):
        here = pl.ds(pl.multiple_of(at * chunk, chunk), chunk)
        vals = []
        high_hots = []
        low_hots = []
        for k in range(3):
            node = corners_ref[pl.ds(k, 1), here]
            height = own if k == 0 else blocks
            high_hot = block_ids[:height] == (node >> shift)
            low_hot = lane_ids == (node & (columns - 1))
            high = jnp.where(high_hot, 1.0, 0.0).astype(jnp.bfloat16)
            picked = jnp.dot(
                tables[min(k, 1)],
                jnp.concatenate([high] * PIECES, axis=0),
                preferred_element_type=jnp.float32,
            )
            vals.append(jnp.sum(jnp.where(low_hot, picked, 0.0), axis=0, keepdims=True))
            high_hots.append(high_hot)
            low_hots.append(low_hot)
        gx0, gy0, gx1, gy1 = (grad_ref[pl.ds(k, 1), here] for k in range(4))
        area = area_ref[:, here]
        scaled = depth_ref[:, here] * area
        third = area * (1.0 / 3.0)
        d0 = vals[0] - vals[2]
        d1 = vals[1] - vals[2]
        flux_x = scaled * (gx0 * d0 + gx1 * d1)
        flux_y = scaled * (gy0 * d0 + gy1 * d1)
        y0 = gx0 * flux_x + gy0 * flux_y
        y1 = gx1 * flux_x + gy1 * flux_y
        outs = [y0 + third * vals[0], y1 + third * vals[1], third * vals[2] - (y0 + y1)]
        accs = list(accs)
        for k in range(3):
            left = jnp.concatenate(
                [
                    jnp.where(high_hots[k], piece.astype(jnp.float32), 0.0).astype(jnp.bfloat16)
                    for piece in split(outs[k])
                ],
                axis=0,
            )
            right = jnp.where(low_hots[k], 1.0, 0.0).astype(jnp.bfloat16)
            accs[min(k, 1)] = accs[min(k, 1)] + lax.dot_general(
                left, right, (((1,), (1,)), ((), ())), preferred_element_type=jnp.float32
            )
        return tuple(accs)

    accs = lax.fori_loop(
        0,
        corners_ref.shape[1] // chunk,
        step,
        (
            jnp.zeros((PIECES * own, columns), jnp.float32),
            jnp.zeros((PIECES * blocks, columns), jnp.float32),
        ),
    )

    def joined(acc, height):
        total = acc[:height]
        for piece in range(1, PIECES):
            total = total + acc[piece * height : (piece + 1) * height]
        return total

    summed = joined(accs[1], blocks)
    own_ref[...] = summed[:own] + joined(accs[0], own)
    packed = exact_dot(recv_hot.T, summed[own:])
    write_messages(flags_ref, packed, shifts, out_refs)


def merge(shifts, flags_ref, own_ref, send_ref, in_refs):
    hot = rows_hot(send_ref[...], own_ref.shape[0])
    incoming = read_messages(flags_ref, shifts, in_refs)
    return own_ref[...] + exact_dot(hot, incoming), hot


def merge_kernel(shifts, subtract, flags_ref, forcing_ref, own_ref, send_ref, *rest):
    in_refs, total_ref, out_refs = rest[:3], rest[3], rest[4:]
    total, hot = merge(shifts, flags_ref, own_ref, send_ref, in_refs)
    if subtract:
        total = forcing_ref[...] - total
    total_ref[...] = total
    packed = exact_dot(hot.T, total)
    write_messages(flags_ref, packed, [-k for k in shifts], out_refs)


def folded(values):
    return jnp.sum(values, axis=0, keepdims=True)


def dots_kernel(shifts, flags_ref, v0_ref, v1_ref, own_ref, send_ref, *rest):
    in_refs, v2_ref, sums_ref = rest[:3], rest[3], rest[4]
    v2, _ = merge(shifts, flags_ref, own_ref, send_ref, in_refs)
    v2_ref[...] = v2
    v0 = v0_ref[...]
    v1 = v1_ref[...]
    rows = [folded(v0 * v0), folded(v0 * v1), folded(v1 * v1), folded(v1 * v2), folded(v0 * v2)]
    rows += [jnp.zeros_like(rows[0])] * (sums_ref.shape[1] - len(rows))
    sums_ref[...] = jnp.broadcast_to(jnp.concatenate(rows, axis=0)[None], sums_ref.shape)


def finish_kernel(guess_ref, v0_ref, v1_ref, v2_ref, sums_ref, elevation_ref, residual_ref):
    devices = sums_ref.shape[0]
    total = sums_ref[0]
    for at in range(1, devices):
        total = total + sums_ref[at]
    each = jnp.sum(total, axis=1, keepdims=True)
    s00, s01, s11, s12, s02 = (each[k : k + 1] for k in range(5))
    a0 = s00 / s01
    rr1 = s00 - a0 * (s01 + s01) + a0 * a0 * s11
    beta = rr1 / s00
    crossed = s01 - a0 * (s11 + s02) + a0 * a0 * s12
    a1 = rr1 / (crossed - beta * rr1 / a0)
    v0 = v0_ref[...]
    v1 = v1_ref[...]
    r1 = v0 - a0 * v1
    p1 = r1 + beta * v0
    image = (v1 - a0 * v2_ref[...]) + beta * v1
    elevation_ref[...] = guess_ref[...] + a0 * v0 + a1 * p1
    residual_ref[...] = r1 - a1 * image


def local(
    forcing, first_guess, corners, gradients, element_area, element_depth, send_blocks, recv_blocks
):
    own, columns = forcing.shape
    offsets = send_blocks.shape[1]
    slots = send_blocks.shape[2]
    shifts = shift_list(offsets)
    send = send_blocks.reshape(1, offsets * slots)
    recv = recv_blocks.reshape(1, offsets * slots)
    elements = corners.shape[1]
    area = element_area.reshape(1, elements)
    depth = element_depth.reshape(1, elements)
    chunk = CHUNK
    block = jax.ShapeDtypeStruct((own, columns), jnp.float32)
    messages = [jax.ShapeDtypeStruct((rows, columns), jnp.float32) for rows in (2 * slots, 2 * slots, slots)]
    devices = lax.axis_size("dom")
    me = lax.axis_index("dom")
    even_core = 1 - me % 2
    even_chip = 1 - (me // 2) % 2
    flags = jnp.stack([even_core, even_chip]).astype(jnp.int32)
    vmem = pl.BlockSpec(memory_space=pltpu.VMEM)
    smem = pl.BlockSpec(memory_space=pltpu.SMEM)

    def call(body, shapes, *operands):
        return pl.pallas_call(
            body, out_shape=shapes, in_specs=[smem] + [vmem] * len(operands)
        )(flags, *operands)

    def exchange(sent):
        first, second, near = sent
        first = paired_swap(first, "dom", 2, 0)
        second = paired_swap(second, "dom", 2, 1)
        far = jnp.where(even_core == even_chip, first[slots:], second[slots:])
        partner = paired_swap(jnp.concatenate([near, far], axis=0), "dom", 1, 0)
        return first, second, partner

    def applied(field, sent):
        own_part, *outgoing = call(
            functools.partial(apply_kernel, chunk, shifts),
            [block] + messages,
            field, recv, corners, gradients, area, depth, *exchange(sent),
        )
        return own_part, exchange(outgoing)

    def merged(own_part, incoming, subtract):
        total, *outgoing = call(
            functools.partial(merge_kernel, shifts, subtract),
            [block] + messages,
            forcing, own_part, send, *incoming,
        )
        return total, outgoing

    outgoing = call(functools.partial(pack_kernel, shifts), messages, first_guess, send)
    v0, outgoing = merged(*applied(first_guess, outgoing), True)
    v1, outgoing = merged(*applied(v0, outgoing), False)
    own_part, incoming = applied(v1, outgoing)
    v2, sums = call(
        functools.partial(dots_kernel, shifts),
        [block, jax.ShapeDtypeStruct((devices, 8, columns), jnp.float32)],
        v0, v1, own_part, send, *incoming,
    )
    gathered = lax.all_to_all(sums, "dom", 0, 0)
    return tuple(
        pl.pallas_call(finish_kernel, out_shape=[block, block])(
            first_guess, v0, v1, v2, gathered
        )
    )


def solution(mesh):
    placed = (
        P("dom", None),
        P("dom", None),
        P(None, "dom"),
        P(None, "dom"),
        P("dom"),
        P("dom"),
        P("dom", None, None),
        P("dom", None, None),
    )
    return jax.shard_map(
        local,
        mesh=mesh,
        in_specs=placed,
        out_specs=(P("dom", None), P("dom", None)),
        check_vma=False,
    )
```

```python
import functools

import jax
import jax.numpy as jnp
from jax import lax
from jax.experimental import pallas as pl
from jax.experimental.pallas import tpu as pltpu
from jax.sharding import PartitionSpec as P

ITERS = 2
PIECES = 2
CHUNK = 4096


def paired_swap(block, axis, reach, odd):
    count = lax.axis_size(axis)
    route = []
    for low in range(count - reach):
        if (low // reach) % 2 == odd:
            route += [(low, low + reach), (low + reach, low)]
    return lax.ppermute(block, axis, route)


def shift_list(offsets):
    half_count = offsets // 2
    return [
        shift_at - half_count if shift_at < half_count else shift_at - half_count + 1
        for shift_at in range(offsets)
    ]


def exact_dot(left, right):
    return jnp.dot(left, right, precision=lax.Precision.HIGHEST, preferred_element_type=jnp.float32)


def split(values):
    pieces = []
    for _ in range(PIECES):
        piece = values.astype(jnp.bfloat16)
        pieces.append(piece)
        values = values - piece.astype(jnp.float32)
    return pieces


def rows_hot(table, count):
    return (
        lax.broadcasted_iota(jnp.int32, (count, table.shape[1]), 0) == table
    ).astype(jnp.float32)


def chosen(flag, yes, no):
    return jnp.where(jnp.full(yes.shape, flag, jnp.int32) == 1, yes, no)


def write_messages(flags_ref, packed, toward, refs):
    slots = packed.shape[0] // len(toward)
    to = {t: packed[at * slots : (at + 1) * slots] for at, t in enumerate(toward)}
    up = jnp.concatenate([to[2], to[1]], axis=0)
    down = jnp.concatenate([to[-2], to[-1]], axis=0)
    even_core, even_chip = flags_ref[0], flags_ref[1]
    refs[0][...] = chosen(even_chip, up, down)
    refs[1][...] = chosen(even_chip, down, up)
    refs[2][...] = chosen(even_core, to[1], to[-1])


def read_messages(flags_ref, toward, refs):
    first, second, near, relay_first, relay_second = (ref[...] for ref in refs)
    slots = near.shape[0]
    even_core, even_chip = flags_ref[0], flags_ref[1]
    far = chosen(
        jnp.where(even_core == even_chip, 1, 0), relay_second[slots:], relay_first[slots:]
    )
    got = {
        2: chosen(even_chip, second[:slots], first[:slots]),
        -2: chosen(even_chip, first[:slots], second[:slots]),
        1: chosen(even_core, far, near),
        -1: chosen(even_core, near, far),
    }
    return jnp.concatenate([got[t] for t in toward], axis=0)


def pack_kernel(shifts, flags_ref, x_ref, send_ref, *out_refs):
    hot = rows_hot(send_ref[...], x_ref.shape[0])
    packed = exact_dot(hot.T, x_ref[...])
    write_messages(flags_ref, packed, [-k for k in shifts], out_refs)


def apply_kernel(
    chunk, shifts, flags_ref, x_ref, recv_ref, corners_ref, grad_ref, area_ref, depth_ref, *rest
):
    in_refs, own_ref, out_refs = rest[:5], rest[5], rest[6:]
    own, columns = x_ref.shape
    halo = recv_ref.shape[1]
    blocks = own + halo
    shift = columns.bit_length() - 1
    recv_hot = rows_hot(recv_ref[...], halo)
    incoming = read_messages(flags_ref, [-k for k in shifts], in_refs)
    field = jnp.concatenate([x_ref[...], exact_dot(recv_hot, incoming)], axis=0)
    field_pieces = split(field)
    tables = [
        jnp.concatenate([piece[:height] for piece in field_pieces], axis=0)
        for height in (own, blocks)
    ]
    block_ids = lax.broadcasted_iota(jnp.int32, (blocks, chunk), 0)
    assert max(columns, blocks) <= 256
    lane_ids = lax.broadcasted_iota(jnp.int32, (columns, chunk), 0)
    lane_ids = lane_ids.astype(jnp.float32).astype(jnp.bfloat16)
    block_nums = block_ids.astype(jnp.float32).astype(jnp.bfloat16)
    one = jnp.ones((), jnp.bfloat16)
    zero = jnp.zeros((), jnp.bfloat16)

    def step(at, accs):
        here = pl.ds(pl.multiple_of(at * chunk, chunk), chunk)
        vals = []
        high_hots = []
        low_hots = []
        for k in range(3):
            node = corners_ref[pl.ds(k, 1), here]
            height = own if k == 0 else blocks
            high_hot = block_ids[:height] == (node >> shift)
            low = (node & (columns - 1)).astype(jnp.float32).astype(jnp.bfloat16)
            low_hot = jnp.where(lane_ids == low, one, zero)
            picked = jnp.dot(tables[min(k, 1)], low_hot, preferred_element_type=jnp.float32)
            rows = picked[:height]
            for piece in range(1, PIECES):
                rows = rows + picked[piece * height : (piece + 1) * height]
            vals.append(jnp.sum(jnp.where(high_hot, rows, 0.0), axis=0, keepdims=True))
            high = (node >> shift).astype(jnp.float32).astype(jnp.bfloat16)
            high_hots.append(block_nums[:height] == high)
            low_hots.append(low_hot)
        gx0, gy0, gx1, gy1 = (grad_ref[pl.ds(k, 1), here] for k in range(4))
        area = area_ref[:, here]
        scaled = depth_ref[:, here] * area
        third = area * (1.0 / 3.0)
        d0 = vals[0] - vals[2]
        d1 = vals[1] - vals[2]
        flux_x = scaled * (gx0 * d0 + gx1 * d1)
        flux_y = scaled * (gy0 * d0 + gy1 * d1)
        y0 = gx0 * flux_x + gy0 * flux_y
        y1 = gx1 * flux_x + gy1 * flux_y
        outs = [y0 + third * vals[0], y1 + third * vals[1], third * vals[2] - (y0 + y1)]
        accs = list(accs)
        for k in range(3):
            left = jnp.concatenate(
                [
                    jnp.where(high_hots[k], piece, zero)
                    for piece in split(outs[k])
                ],
                axis=0,
            )
            accs[min(k, 1)] = accs[min(k, 1)] + lax.dot_general(
                left, low_hots[k], (((1,), (1,)), ((), ())), preferred_element_type=jnp.float32
            )
        return tuple(accs)

    accs = lax.fori_loop(
        0,
        corners_ref.shape[1] // chunk,
        step,
        (
            jnp.zeros((PIECES * own, columns), jnp.float32),
            jnp.zeros((PIECES * blocks, columns), jnp.float32),
        ),
    )

    def joined(acc, height):
        total = acc[:height]
        for piece in range(1, PIECES):
            total = total + acc[piece * height : (piece + 1) * height]
        return total

    summed = joined(accs[1], blocks)
    own_ref[...] = summed[:own] + joined(accs[0], own)
    packed = exact_dot(recv_hot.T, summed[own:])
    write_messages(flags_ref, packed, shifts, out_refs)


def merge(shifts, flags_ref, own_ref, send_ref, in_refs):
    hot = rows_hot(send_ref[...], own_ref.shape[0])
    incoming = read_messages(flags_ref, shifts, in_refs)
    return own_ref[...] + exact_dot(hot, incoming), hot


def merge_kernel(shifts, subtract, flags_ref, forcing_ref, own_ref, send_ref, *rest):
    in_refs, total_ref, out_refs = rest[:5], rest[5], rest[6:]
    total, hot = merge(shifts, flags_ref, own_ref, send_ref, in_refs)
    if subtract:
        total = forcing_ref[...] - total
    total_ref[...] = total
    packed = exact_dot(hot.T, total)
    write_messages(flags_ref, packed, [-k for k in shifts], out_refs)


def folded(values):
    return jnp.sum(values, axis=0, keepdims=True)


def dots_kernel(shifts, flags_ref, v0_ref, v1_ref, own_ref, send_ref, *rest):
    in_refs, v2_ref, sums_ref = rest[:5], rest[5], rest[6]
    v2, _ = merge(shifts, flags_ref, own_ref, send_ref, in_refs)
    v2_ref[...] = v2
    v0 = v0_ref[...]
    v1 = v1_ref[...]
    rows = [folded(v0 * v0), folded(v0 * v1), folded(v1 * v1), folded(v1 * v2), folded(v0 * v2)]
    rows += [jnp.zeros_like(rows[0])] * (sums_ref.shape[1] - len(rows))
    sums_ref[...] = jnp.broadcast_to(jnp.concatenate(rows, axis=0)[None], sums_ref.shape)


def finish_kernel(guess_ref, v0_ref, v1_ref, v2_ref, sums_ref, elevation_ref, residual_ref):
    devices = sums_ref.shape[0]
    total = sums_ref[0]
    for at in range(1, devices):
        total = total + sums_ref[at]
    each = jnp.sum(total, axis=1, keepdims=True)
    s00, s01, s11, s12, s02 = (each[k : k + 1] for k in range(5))
    a0 = s00 / s01
    rr1 = s00 - a0 * (s01 + s01) + a0 * a0 * s11
    beta = rr1 / s00
    crossed = s01 - a0 * (s11 + s02) + a0 * a0 * s12
    a1 = rr1 / (crossed - beta * rr1 / a0)
    v0 = v0_ref[...]
    v1 = v1_ref[...]
    r1 = v0 - a0 * v1
    p1 = r1 + beta * v0
    image = (v1 - a0 * v2_ref[...]) + beta * v1
    elevation_ref[...] = guess_ref[...] + a0 * v0 + a1 * p1
    residual_ref[...] = r1 - a1 * image


def local(
    forcing, first_guess, corners, gradients, element_area, element_depth, send_blocks, recv_blocks
):
    own, columns = forcing.shape
    offsets = send_blocks.shape[1]
    slots = send_blocks.shape[2]
    shifts = shift_list(offsets)
    send = send_blocks.reshape(1, offsets * slots)
    recv = recv_blocks.reshape(1, offsets * slots)
    elements = corners.shape[1]
    area = element_area.reshape(1, elements)
    depth = element_depth.reshape(1, elements)
    chunk = CHUNK
    block = jax.ShapeDtypeStruct((own, columns), jnp.float32)
    messages = [jax.ShapeDtypeStruct((rows, columns), jnp.float32) for rows in (2 * slots, 2 * slots, slots)]
    devices = lax.axis_size("dom")
    me = lax.axis_index("dom")
    even_core = 1 - me % 2
    even_chip = 1 - (me // 2) % 2
    flags = jnp.stack([even_core, even_chip]).astype(jnp.int32)
    vmem = pl.BlockSpec(memory_space=pltpu.VMEM)
    smem = pl.BlockSpec(memory_space=pltpu.SMEM)

    def call(body, shapes, *operands):
        return pl.pallas_call(
            body, out_shape=shapes, in_specs=[smem] + [vmem] * len(operands)
        )(flags, *operands)

    def exchange(sent):
        first, second, near = sent
        near = paired_swap(near, "dom", 1, 0)
        first = paired_swap(first, "dom", 2, 0)
        second = paired_swap(second, "dom", 2, 1)
        relayed = [paired_swap(part, "dom", 1, 0) for part in (first, second)]
        return first, second, near, *relayed

    def applied(field, sent):
        own_part, *outgoing = call(
            functools.partial(apply_kernel, chunk, shifts),
            [block] + messages,
            field, recv, corners, gradients, area, depth, *exchange(sent),
        )
        return own_part, exchange(outgoing)

    def merged(own_part, incoming, subtract):
        total, *outgoing = call(
            functools.partial(merge_kernel, shifts, subtract),
            [block] + messages,
            forcing, own_part, send, *incoming,
        )
        return total, outgoing

    outgoing = call(functools.partial(pack_kernel, shifts), messages, first_guess, send)
    v0, outgoing = merged(*applied(first_guess, outgoing), True)
    v1, outgoing = merged(*applied(v0, outgoing), False)
    own_part, incoming = applied(v1, outgoing)
    v2, sums = call(
        functools.partial(dots_kernel, shifts),
        [block, jax.ShapeDtypeStruct((devices, 8, columns), jnp.float32)],
        v0, v1, own_part, send, *incoming,
    )
    gathered = lax.all_to_all(sums, "dom", 0, 0)
    return tuple(
        pl.pallas_call(finish_kernel, out_shape=[block, block])(
            first_guess, v0, v1, v2, gathered
        )
    )


def solution(mesh):
    placed = (
        P("dom", None),
        P("dom", None),
        P(None, "dom"),
        P(None, "dom"),
        P("dom"),
        P("dom"),
        P("dom", None, None),
        P("dom", None, None),
    )
    return jax.shard_map(
        local,
        mesh=mesh,
        in_specs=placed,
        out_specs=(P("dom", None), P("dom", None)),
        check_vma=False,
    )
```

```python
import functools

import jax
import jax.numpy as jnp
from jax import lax
from jax.experimental import pallas as pl
from jax.experimental.pallas import tpu as pltpu
from jax.sharding import PartitionSpec as P

ITERS = 2
PIECES = 2


def paired_swap(block, axis, reach, odd):
    count = lax.axis_size(axis)
    route = []
    for low in range(count - reach):
        if (low // reach) % 2 == odd:
            route += [(low, low + reach), (low + reach, low)]
    return lax.ppermute(block, axis, route)


def shift_list(offsets):
    half_count = offsets // 2
    return [
        shift_at - half_count if shift_at < half_count else shift_at - half_count + 1
        for shift_at in range(offsets)
    ]


def exact_dot(left, right):
    return jnp.dot(left, right, precision=lax.Precision.HIGHEST, preferred_element_type=jnp.float32)


def split(values):
    pieces = []
    for _ in range(PIECES):
        piece = values.astype(jnp.bfloat16)
        pieces.append(piece)
        values = values - piece.astype(jnp.float32)
    return pieces


def rows_hot(table, count):
    return (
        lax.broadcasted_iota(jnp.int32, (count, table.shape[1]), 0) == table
    ).astype(jnp.float32)


def chosen(flag, yes, no):
    return jnp.where(jnp.full(yes.shape, flag, jnp.int32) == 1, yes, no)


def write_messages(flags_ref, packed, toward, refs):
    slots = packed.shape[0] // len(toward)
    to = {t: packed[at * slots : (at + 1) * slots] for at, t in enumerate(toward)}
    up = jnp.concatenate([to[2], to[1]], axis=0)
    down = jnp.concatenate([to[-2], to[-1]], axis=0)
    even_core, even_chip = flags_ref[0], flags_ref[1]
    refs[0][...] = chosen(even_chip, up, down)
    refs[1][...] = chosen(even_chip, down, up)
    refs[2][...] = chosen(even_core, to[1], to[-1])


def read_messages(flags_ref, toward, refs):
    first, second, near, relay_first, relay_second = (ref[...] for ref in refs)
    slots = near.shape[0]
    even_core, even_chip = flags_ref[0], flags_ref[1]
    far = chosen(
        jnp.where(even_core == even_chip, 1, 0), relay_second[slots:], relay_first[slots:]
    )
    got = {
        2: chosen(even_chip, second[:slots], first[:slots]),
        -2: chosen(even_chip, first[:slots], second[:slots]),
        1: chosen(even_core, far, near),
        -1: chosen(even_core, near, far),
    }
    return jnp.concatenate([got[t] for t in toward], axis=0)


def pack_kernel(shifts, flags_ref, x_ref, send_ref, *out_refs):
    hot = rows_hot(send_ref[...], x_ref.shape[0])
    packed = exact_dot(hot.T, x_ref[...])
    write_messages(flags_ref, packed, [-k for k in shifts], out_refs)


def apply_kernel(
    chunk, shifts, flags_ref, x_ref, recv_ref, corners_ref, grad_ref, area_ref, depth_ref, *rest
):
    in_refs, own_ref, out_refs = rest[:5], rest[5], rest[6:]
    own, columns = x_ref.shape
    halo = recv_ref.shape[1]
    blocks = own + halo
    shift = columns.bit_length() - 1
    recv_hot = rows_hot(recv_ref[...], halo)
    incoming = read_messages(flags_ref, [-k for k in shifts], in_refs)
    field = jnp.concatenate([x_ref[...], exact_dot(recv_hot, incoming)], axis=0)
    field_pieces = split(field)
    tables = [
        jnp.concatenate([piece[:height] for piece in field_pieces], axis=0)
        for height in (own, blocks)
    ]
    block_ids = lax.broadcasted_iota(jnp.int32, (blocks, chunk), 0)
    assert max(columns, blocks) <= 256
    lane_ids = lax.broadcasted_iota(jnp.int32, (columns, chunk), 0)
    lane_ids = lane_ids.astype(jnp.float32).astype(jnp.bfloat16)
    block_nums = block_ids.astype(jnp.float32).astype(jnp.bfloat16)
    one = jnp.ones((), jnp.bfloat16)
    zero = jnp.zeros((), jnp.bfloat16)

    def step(at, accs):
        here = pl.ds(pl.multiple_of(at * chunk, chunk), chunk)
        vals = []
        high_hots = []
        low_hots = []
        for k in range(3):
            node = corners_ref[pl.ds(k, 1), here]
            height = own if k == 0 else blocks
            high_hot = block_ids[:height] == (node >> shift)
            low = (node & (columns - 1)).astype(jnp.float32).astype(jnp.bfloat16)
            low_hot = jnp.where(lane_ids == low, one, zero)
            picked = jnp.dot(tables[min(k, 1)], low_hot, preferred_element_type=jnp.float32)
            rows = picked[:height]
            for piece in range(1, PIECES):
                rows = rows + picked[piece * height : (piece + 1) * height]
            vals.append(jnp.sum(jnp.where(high_hot, rows, 0.0), axis=0, keepdims=True))
            high = (node >> shift).astype(jnp.float32).astype(jnp.bfloat16)
            high_hots.append(block_nums[:height] == high)
            low_hots.append(low_hot)
        gx0, gy0, gx1, gy1 = (grad_ref[pl.ds(k, 1), here] for k in range(4))
        area = area_ref[:, here]
        scaled = depth_ref[:, here] * area
        third = area * (1.0 / 3.0)
        d0 = vals[0] - vals[2]
        d1 = vals[1] - vals[2]
        flux_x = scaled * (gx0 * d0 + gx1 * d1)
        flux_y = scaled * (gy0 * d0 + gy1 * d1)
        y0 = gx0 * flux_x + gy0 * flux_y
        y1 = gx1 * flux_x + gy1 * flux_y
        outs = [y0 + third * vals[0], y1 + third * vals[1], third * vals[2] - (y0 + y1)]
        accs = list(accs)
        for k in range(3):
            left = jnp.concatenate(
                [
                    jnp.where(high_hots[k], piece, zero)
                    for piece in split(outs[k])
                ],
                axis=0,
            )
            accs[min(k, 1)] = accs[min(k, 1)] + lax.dot_general(
                left, low_hots[k], (((1,), (1,)), ((), ())), preferred_element_type=jnp.float32
            )
        return tuple(accs)

    accs = lax.fori_loop(
        0,
        corners_ref.shape[1] // chunk,
        step,
        (
            jnp.zeros((PIECES * own, columns), jnp.float32),
            jnp.zeros((PIECES * blocks, columns), jnp.float32),
        ),
    )

    def joined(acc, height):
        total = acc[:height]
        for piece in range(1, PIECES):
            total = total + acc[piece * height : (piece + 1) * height]
        return total

    summed = joined(accs[1], blocks)
    own_ref[...] = summed[:own] + joined(accs[0], own)
    packed = exact_dot(recv_hot.T, summed[own:])
    write_messages(flags_ref, packed, shifts, out_refs)


def merge(shifts, flags_ref, own_ref, send_ref, in_refs):
    hot = rows_hot(send_ref[...], own_ref.shape[0])
    incoming = read_messages(flags_ref, shifts, in_refs)
    return own_ref[...] + exact_dot(hot, incoming), hot


def merge_kernel(shifts, subtract, flags_ref, forcing_ref, own_ref, send_ref, *rest):
    in_refs, total_ref, out_refs = rest[:5], rest[5], rest[6:]
    total, hot = merge(shifts, flags_ref, own_ref, send_ref, in_refs)
    if subtract:
        total = forcing_ref[...] - total
    total_ref[...] = total
    packed = exact_dot(hot.T, total)
    write_messages(flags_ref, packed, [-k for k in shifts], out_refs)


def folded(values):
    return jnp.sum(values, axis=0, keepdims=True)


def dots_kernel(shifts, flags_ref, v0_ref, v1_ref, own_ref, send_ref, *rest):
    in_refs, v2_ref, sums_ref = rest[:5], rest[5], rest[6]
    v2, _ = merge(shifts, flags_ref, own_ref, send_ref, in_refs)
    v2_ref[...] = v2
    v0 = v0_ref[...]
    v1 = v1_ref[...]
    rows = [folded(v0 * v0), folded(v0 * v1), folded(v1 * v1), folded(v1 * v2), folded(v0 * v2)]
    rows += [jnp.zeros_like(rows[0])] * (sums_ref.shape[1] - len(rows))
    sums_ref[...] = jnp.broadcast_to(jnp.concatenate(rows, axis=0)[None], sums_ref.shape)


def finish_kernel(guess_ref, v0_ref, v1_ref, v2_ref, sums_ref, elevation_ref, residual_ref):
    devices = sums_ref.shape[0]
    total = sums_ref[0]
    for at in range(1, devices):
        total = total + sums_ref[at]
    each = jnp.sum(total, axis=1, keepdims=True)
    s00, s01, s11, s12, s02 = (each[k : k + 1] for k in range(5))
    a0 = s00 / s01
    rr1 = s00 - a0 * (s01 + s01) + a0 * a0 * s11
    beta = rr1 / s00
    crossed = s01 - a0 * (s11 + s02) + a0 * a0 * s12
    a1 = rr1 / (crossed - beta * rr1 / a0)
    v0 = v0_ref[...]
    v1 = v1_ref[...]
    r1 = v0 - a0 * v1
    p1 = r1 + beta * v0
    image = (v1 - a0 * v2_ref[...]) + beta * v1
    elevation_ref[...] = guess_ref[...] + a0 * v0 + a1 * p1
    residual_ref[...] = r1 - a1 * image


def local(
    forcing, first_guess, corners, gradients, element_area, element_depth, send_blocks, recv_blocks
):
    own, columns = forcing.shape
    offsets = send_blocks.shape[1]
    slots = send_blocks.shape[2]
    shifts = shift_list(offsets)
    send = send_blocks.reshape(1, offsets * slots)
    recv = recv_blocks.reshape(1, offsets * slots)
    elements = corners.shape[1]
    area = element_area.reshape(1, elements)
    depth = element_depth.reshape(1, elements)
    chunk = elements
    block = jax.ShapeDtypeStruct((own, columns), jnp.float32)
    messages = [jax.ShapeDtypeStruct((rows, columns), jnp.float32) for rows in (2 * slots, 2 * slots, slots)]
    devices = lax.axis_size("dom")
    me = lax.axis_index("dom")
    even_core = 1 - me % 2
    even_chip = 1 - (me // 2) % 2
    flags = jnp.stack([even_core, even_chip]).astype(jnp.int32)
    vmem = pl.BlockSpec(memory_space=pltpu.VMEM)
    smem = pl.BlockSpec(memory_space=pltpu.SMEM)

    def call(body, shapes, *operands):
        return pl.pallas_call(
            body, out_shape=shapes, in_specs=[smem] + [vmem] * len(operands)
        )(flags, *operands)

    def exchange(sent):
        first, second, near = sent
        near = paired_swap(near, "dom", 1, 0)
        first = paired_swap(first, "dom", 2, 0)
        second = paired_swap(second, "dom", 2, 1)
        relayed = [paired_swap(part, "dom", 1, 0) for part in (first, second)]
        return first, second, near, *relayed

    def applied(field, sent):
        own_part, *outgoing = call(
            functools.partial(apply_kernel, chunk, shifts),
            [block] + messages,
            field, recv, corners, gradients, area, depth, *exchange(sent),
        )
        return own_part, exchange(outgoing)

    def merged(own_part, incoming, subtract):
        total, *outgoing = call(
            functools.partial(merge_kernel, shifts, subtract),
            [block] + messages,
            forcing, own_part, send, *incoming,
        )
        return total, outgoing

    outgoing = call(functools.partial(pack_kernel, shifts), messages, first_guess, send)
    v0, outgoing = merged(*applied(first_guess, outgoing), True)
    v1, outgoing = merged(*applied(v0, outgoing), False)
    own_part, incoming = applied(v1, outgoing)
    v2, sums = call(
        functools.partial(dots_kernel, shifts),
        [block, jax.ShapeDtypeStruct((devices, 8, columns), jnp.float32)],
        v0, v1, own_part, send, *incoming,
    )
    gathered = lax.all_to_all(sums, "dom", 0, 0)
    return tuple(
        pl.pallas_call(finish_kernel, out_shape=[block, block])(
            first_guess, v0, v1, v2, gathered
        )
    )


def solution(mesh):
    placed = (
        P("dom", None),
        P("dom", None),
        P(None, "dom"),
        P(None, "dom"),
        P("dom"),
        P("dom"),
        P("dom", None, None),
        P("dom", None, None),
    )
    return jax.shard_map(
        local,
        mesh=mesh,
        in_specs=placed,
        out_specs=(P("dom", None), P("dom", None)),
        check_vma=False,
    )
```
